128 devices in a mesh: rep: 4 (over x_hi, core), tp: 32 (over z, x_lo, y).
Axes of the slice: x: 4 (x_hi: 2, x_lo: 2; x = x_hi * 2 + x_lo), y: 4, z: 4, core: 2. Of those that a mesh axis runs over, the one named last changes fastest.
Arguments:
- trainer_query: float32 [128, 64, 8192], P(('rep', 'tp')), may hold values from -6 to 6
- trainer_output: float32 [128, 8192, 64], P(('rep', 'tp')), may hold values from -6 to 6
- probes: bfloat16 [768, 8192], replicated, may hold values from -0.0625 to 0.0625
- shard_block: int32 [128], replicated, may hold values from 0 to 127, each once
- slice_owner: int32 [32], replicated, may hold values from 0 to 31, each once
Outputs:
- query_slices: bfloat16 [32, 8192, 256], P('tp')
- output_slices: bfloat16 [32, 256, 8192], P('tp')
- query_prints: float32 [32, 768, 256], P('tp')
- output_prints: float32 [32, 256, 768], P('tp')
The draws below stay inside these ranges and needn't reach their ends.
Inputs may be any that keep to these rules, and one draw needn't show every extreme that they name: `shard_block`: a permutation: each number once. `slice_owner`: a permutation: each number once.
All inputs are finite; a program needn't handle non-finite values.
Results may differ from the reference program's by a relative error of at most 0.0029.
Values may be sent and summed in bfloat16 or wider, within the bound.
A program may use at most 128 MiB of HBM per device.

```python
import jax
import jax.numpy as jnp

D = 8192
PROBES = 768
HQ = 8192
SHARD = 64
SLICE = 256
N_TP = 32
DEVICES = 128


def shard_levels(rng, extent, shards, low, high):
    loudness = 1.0
    for dim, blocks in shards:
        heights = jax.random.uniform(jax.random.fold_in(jax.random.fold_in(rng, 6), dim), (blocks,), jnp.float32, low / len(shards), high / len(shards))
        loudness = loudness * jnp.repeat(jnp.exp(heights), extent[dim] // blocks).reshape((-1,) + (1,) * (len(extent) - 1 - dim))
    return loudness


def noise(stream_key, shape, deviation, reach, shards=(), kind=jnp.bfloat16):
    entries = deviation * jax.random.normal(stream_key, shape, jnp.float32)
    if shards:
        entries = entries * shard_levels(stream_key, shape, shards, -0.22, 0.18)
    return jnp.clip(entries, -reach, reach).astype(kind)


def setup_inputs(seed: int = 0) -> dict:
    streams_of = jax.random.split(jax.random.key(seed), 6)
    return {
        "trainer_query": noise(streams_of[0], (DEVICES, SHARD, HQ), 1.0, 6.0, ((0, 128),), jnp.float32),
        "trainer_output": noise(streams_of[1], (DEVICES, HQ, SHARD), 1.0, 6.0, ((0, 128),), jnp.float32),
        "probes": noise(streams_of[2], (PROBES, D), D ** -0.5, 0.0625),
        "shard_block": jax.random.permutation(streams_of[3], DEVICES).astype(jnp.int32),
        "slice_owner": jax.random.permutation(streams_of[4], N_TP).astype(jnp.int32),
    }


def reference(trainer_query, trainer_output, probes, shard_block, slice_owner):
    positions = jnp.arange(DEVICES, dtype=jnp.int32)
    inverse = jnp.zeros((DEVICES,), jnp.int32).at[shard_block].set(positions)
    query_full = trainer_query.astype(jnp.bfloat16)[inverse].reshape(D, HQ)
    output_full = jnp.transpose(trainer_output.astype(jnp.bfloat16)[inverse], (1, 0, 2)).reshape(HQ, D)
    query_slices = jnp.transpose(query_full.reshape(D, N_TP, SLICE)[:, slice_owner], (1, 0, 2))
    output_slices = output_full.reshape(N_TP, SLICE, D)[slice_owner]
    probe_wide = probes.astype(jnp.float32)
    query_prints = jnp.einsum("pd,jdc->jpc", probe_wide, query_slices.astype(jnp.float32))
    output_prints = jnp.einsum("jcd,pd->jcp", output_slices.astype(jnp.float32), probe_wide)
    return (query_slices, output_slices, query_prints, output_prints)
```

```python
import jax
import jax.numpy as jnp
from jax import lax
from jax.experimental import pallas as pl
from jax.experimental.pallas import tpu as pltpu
from jax.sharding import PartitionSpec as P

MESH = pl.DeviceIdType.MESH
BF16 = jnp.bfloat16
F32 = jnp.float32

ROUNDS = 16
LAG_X = 3
LAG_D = 4


def near_first(i):
    return lax.rem(lax.div(i * (i + 1), 2), 4)


def offset_of(k):
    k = jnp.int32(k)
    return near_first(lax.rem(k, 4)), near_first(lax.div(k, 4))


def place():
    rep, tp = lax.axis_index("rep"), lax.axis_index("tp")
    x = lax.div(rep, 2) * 2 + lax.rem(lax.div(tp, 4), 2)
    return x, lax.rem(tp, 4), lax.div(tp, 8), lax.rem(rep, 2)


def device(x, y, z, core):
    x, y, z = lax.rem(x, 4), lax.rem(y, 4), lax.rem(z, 4)
    return {"rep": lax.div(x, 2) * 2 + core, "tp": z * 8 + lax.rem(x, 2) * 4 + y}


def move_kernel(
    owner, block, query, output, probes,
    recv, turned, prints,
    query_f, output_f, probes_v, staged, relay, lhs, rhs,
    load_sem, probe_sem, near_s, near_r, far_s, far_r, x_s, x_r, d_s, d_r,
):
    x, y, z, core = place()
    mine = z * 4 + y
    barrier = pltpu.get_barrier_semaphore()
    peers = [device(x, y + k % 4, z + k // 4, core) for k in range(1, ROUNDS)]
    peers += [device(x + d, y, z, core) for d in (1, 2, 3)] + [device(x, y, z, 1 - core)]

    def load(kind, i):
        if kind == 2:
            cols = pl.ds(pl.multiple_of(i * 128, 128), 128)
            return pltpu.make_async_copy(probes.at[:, cols], probes_v.at[i], probe_sem.at[i])
        cols = pl.ds(pl.multiple_of(i * 256, 256), 256)
        src, dst = ((query, query_f), (output, output_f))[kind]
        return pltpu.make_async_copy(src.at[:, cols], dst.at[i], load_sem.at[kind, i])

    @pl.loop(0, 32)
    def _(i):
        load(0, i).start()
        load(1, i).start()

    @pl.loop(0, 64)
    def _(i):
        load(2, i).start()

    for peer in peers:
        pl.semaphore_signal(barrier, 1, device_id=peer, device_id_type=MESH)

    def remote(src, dst, send, receive, target):
        return pltpu.make_async_remote_copy(
            src_ref=src, dst_ref=dst, send_sem=send, recv_sem=receive,
            device_id=target, device_id_type=MESH,
        )

    def plane_of(k):
        dy, dz = offset_of(k)
        return lax.rem(z - dz + 4, 4) * 4 + lax.rem(y - dy + 4, 4)

    def near(k):
        dy, dz = offset_of(k)
        return remote(staged.at[k, 0], recv.at[mine, core, x], near_s.at[k], near_r.at[k],
                      device(x, y + dy, z + dz, core))

    def far(k):
        dy, dz = offset_of(k)
        return remote(staged.at[k, 1], relay.at[k], far_s.at[k], far_r.at[k],
                      device(x, y + dy, z + dz, core))

    def along(k):
        own = recv.at[plane_of(k), core, x]
        return (
            remote(relay.at[k], own, x_s.at[k, 0], x_r.at[k, 0], device(x + 1, y, z, core)),
            remote(relay.at[k], own, x_s.at[k, 1], x_r.at[k, 1], device(x + 3, y, z, core)),
            remote(own, own, x_s.at[k, 2], x_r.at[k, 2], device(x + 2, y, z, core)),
        )

    def across(k):
        half = recv.at[plane_of(k), core]
        return remote(half, half, d_s.at[k], d_r.at[k], device(x, y, z, 1 - core))

    def piece(k, other):
        dy, dz = offset_of(k)
        low = lax.rem(x + other, 2)
        j = lax.rem(z + dz, 4) * 8 + low * 4 + lax.rem(y + dy, 4)
        at = owner[j]
        return query_f[at].astype(BF16), output_f[at].astype(BF16)

    @pl.loop(0, 32)
    def _(i):
        load(0, i).wait()
        load(1, i).wait()

    recv[mine, core, x, 0:64, :], recv[mine, core, x, 64:128, :] = piece(0, 0)
    relay[0, 0:64, :], relay[0, 64:128, :] = piece(0, 1)

    def stage(k):
        for other in (0, 1):
            staged[k, other, 0:64, :], staged[k, other, 64:128, :] = piece(k, other)

    stage(1)
    pl.semaphore_wait(barrier, len(peers))
    for copy in along(0):
        copy.start()

    @pl.loop(2, ROUNDS + 1)
    def _(k):
        @pl.when(k < ROUNDS)
        def _():
            stage(k)

        far(k - 1).start()
        near(k - 1).start()

    prints[...] = jnp.zeros_like(prints)

    @pl.loop(0, 64)
    def _(i):
        load(2, i).wait()

    half = lax.div(lax.broadcasted_iota(jnp.int32, (128, 256), 0), 64)

    def compute(k):
        plane = plane_of(k)
        src_z, src_y = lax.div(plane, 4), lax.rem(plane, 4)
        for i in range(8):
            src_c, src_x = i // 4, i % 4
            shard = ((src_x // 2) * 2 + src_c) * 32 + src_z * 8 + (src_x % 2) * 4 + src_y
            at = block[shard]
            lhs[:, i * 128 : (i + 1) * 128] = probes_v[lax.div(at, 2)]
            q = recv[plane, src_c, src_x, 0:64, :]
            o = recv[plane, src_c, src_x, 64:128, :]
            held = half == lax.rem(at, 2)
            for part, data in enumerate((q, o)):
                pair = jnp.concatenate([data, data], axis=0)
                cols = slice(part * 256, (part + 1) * 256)
                rhs[i * 128 : (i + 1) * 128, cols] = jnp.where(held, pair, jnp.zeros_like(pair))
            turned[plane * 8 + i] = jnp.concatenate([o, o], axis=0).T

        @pl.loop(0, 3)
        def _(m):
            rows = pl.ds(pl.multiple_of(m * 256, 256), 256)
            prints[rows, :] += jnp.dot(lhs[rows, :], rhs[...], preferred_element_type=F32)

    @pl.loop(0, ROUNDS + LAG_D)
    def _(t):
        @pl.when((t >= 1) & (t < ROUNDS))
        def _():
            far(t).wait_recv()
            first, second, third = along(t)
            first.start()
            second.start()
            near(t).wait_recv()
            third.start()

        @pl.when((t >= LAG_X) & (t < ROUNDS + LAG_X))
        def _():
            for copy in along(t - LAG_X):
                copy.wait_recv()
            across(t - LAG_X).start()

        @pl.when(t >= LAG_D)
        def _():
            across(t - LAG_D).wait_recv()
            compute(t - LAG_D)

    @pl.loop(0, ROUNDS)
    def _(k):
        @pl.when(k >= 1)
        def _():
            near(k).wait_send()
            far(k).wait_send()

        for copy in along(k):
            copy.wait_send()
        across(k).wait_send()


def place_kernel(block, recv, turned, prints, q_out, o_out, qp_out, op_out,
                 slot_of, o_all, op_all, sems):
    qp = pltpu.make_async_copy(prints.at[:, 0:256], qp_out, sems.at[1])
    qp.start()

    @pl.loop(0, 128)
    def _(g):
        plane, src_c, src_x = g // 8, (g // 4) % 2, g % 4
        shard = ((src_x // 2) * 2 + src_c) * 32 + (plane // 4) * 8 + (src_x % 2) * 4 + plane % 4
        at = block[shard]
        slot_of[at] = g
        pltpu.make_async_copy(
            recv.at[plane, src_c, src_x, 0:64, :], q_out.at[pl.ds(pl.multiple_of(at * 64, 64), 64), :], sems.at[0]
        ).start()

    left = lax.broadcasted_iota(jnp.int32, (256, 128), 1) < 64
    outs = []
    for part in range(4):
        @pl.loop(part * 16, (part + 1) * 16)
        def _(p):
            one = turned[slot_of[2 * p]]
            two = turned[slot_of[2 * p + 1]]
            o_all[:, pl.ds(pl.multiple_of(p * 128, 128), 128)] = jnp.where(left, one, two)

        cols = slice(part * 2048, (part + 1) * 2048)
        copy = pltpu.make_async_copy(o_all.at[:, cols], o_out.at[:, cols], sems.at[3 + part])
        copy.start()
        outs.append(copy)
    op_all[...] = prints[:, 256:512].T
    op = pltpu.make_async_copy(op_all, op_out, sems.at[2])
    op.start()
    for copy in [qp, op] + outs:
        copy.wait()
    pltpu.make_async_copy(q_out, q_out, sems.at[0]).wait()


def per_device(trainer_query, trainer_output, probes, shard_block, slice_owner):
    smem = pl.BlockSpec(memory_space=pltpu.SMEM)
    hbm = pl.BlockSpec(memory_space=pl.ANY)
    vmem = pl.BlockSpec(memory_space=pltpu.VMEM)
    dma = pltpu.SemaphoreType.DMA
    recv, turned, prints = pl.pallas_call(
        move_kernel,
        out_shape=(
            pltpu.VMEM((16, 2, 4, 128, 256), BF16),
            pltpu.VMEM((128, 256, 128), BF16),
            pltpu.VMEM((768, 512), F32),
        ),
        in_specs=[smem, smem, hbm, hbm, hbm],
        out_specs=(vmem, vmem, vmem),
        scratch_shapes=[
            pltpu.VMEM((32, 64, 256), F32),
            pltpu.VMEM((32, 64, 256), F32),
            pltpu.VMEM((64, 768, 128), BF16),
            pltpu.VMEM((ROUNDS, 2, 128, 256), BF16),
            pltpu.VMEM((ROUNDS, 128, 256), BF16),
            pltpu.VMEM((768, 1024), BF16),
            pltpu.VMEM((1024, 512), BF16),
            dma((2, 32)), dma((64,)), dma((ROUNDS,)), dma((ROUNDS,)), dma((ROUNDS,)), dma((ROUNDS,)),
            dma((ROUNDS, 3)), dma((ROUNDS, 3)), dma((ROUNDS,)), dma((ROUNDS,)),
        ],
        compiler_params=pltpu.CompilerParams(
            collective_id=0, has_side_effects=True, vmem_limit_bytes=44 << 20
        ),
        name="move",
    )(
        slice_owner, shard_block, trainer_query[0], jnp.swapaxes(trainer_output, 1, 2)[0], probes
    )
    outs = pl.pallas_call(
        place_kernel,
        out_shape=(
            jax.ShapeDtypeStruct((8192, 256), BF16),
            jax.ShapeDtypeStruct((256, 8192), BF16),
            jax.ShapeDtypeStruct((768, 256), F32),
            jax.ShapeDtypeStruct((256, 768), F32),
        ),
        in_specs=[smem, vmem, vmem, vmem],
        out_specs=(hbm, hbm, hbm, hbm),
        scratch_shapes=[
            pltpu.SMEM((128,), jnp.int32),
            pltpu.VMEM((256, 8192), BF16),
            pltpu.VMEM((256, 768), F32),
            dma((8,)),
        ],
        compiler_params=pltpu.CompilerParams(vmem_limit_bytes=32 << 20),
        name="place",
    )(shard_block, recv, turned, prints)
    return tuple(out[None] for out in outs)


def solution(mesh):
    placed = (P(("rep", "tp"), None, None), P(("rep", "tp"), None, None), P(), P(), P())
    return jax.shard_map(
        per_device,
        mesh=mesh,
        in_specs=placed,
        out_specs=(
            P("tp", None, None),
            P("tp", None, None),
            P("tp", None, None),
            P("tp", None, None),
        ),
        check_vma=False,
    )
```

```python
import jax
import jax.numpy as jnp
from jax import lax
from jax.experimental import pallas as pl
from jax.experimental.pallas import tpu as pltpu
from jax.sharding import PartitionSpec as P

MESH = pl.DeviceIdType.MESH
BF16 = jnp.bfloat16
F32 = jnp.float32

ROUNDS = 16
LAG_X = 3
LAG_D = 4
DIRECT = 0


def near_first(i):
    return lax.rem(lax.div(i * (i + 1), 2), 4)


def offset_of(k):
    k = jnp.int32(k)
    return near_first(lax.rem(k, 4)), near_first(lax.div(k, 4))


def place():
    rep, tp = lax.axis_index("rep"), lax.axis_index("tp")
    x = lax.div(rep, 2) * 2 + lax.rem(lax.div(tp, 4), 2)
    return x, lax.rem(tp, 4), lax.div(tp, 8), lax.rem(rep, 2)


def device(x, y, z, core):
    x, y, z = lax.rem(x, 4), lax.rem(y, 4), lax.rem(z, 4)
    return {"rep": lax.div(x, 2) * 2 + core, "tp": z * 8 + lax.rem(x, 2) * 4 + y}


def move_kernel(
    owner, block, block_row, query, output, probes,
    recv, turned, prints, slot_of,
    query_f, output_f, probes_v, staged, relay, lhs, rhs,
    load_sem, probe_sem, near_s, near_r, far_s, far_r, x_s, x_r, d_s, d_r,
):
    x, y, z, core = place()
    mine = z * 4 + y
    barrier = pltpu.get_barrier_semaphore()
    peers = [device(x, y + k % 4, z + k // 4, core) for k in range(1, ROUNDS)]
    peers += [device(x + d, y, z, core) for d in (1, 2, 3)] + [device(x, y, z, 1 - core)]
    if DIRECT:
        peers += [device(x + d, y + 2, z + 2, core) for d in (1, 2, 3)]

    def load(kind, i):
        src, dst = ((query, query_f), (output, output_f))[kind]
        return pltpu.make_async_copy(src.at[i], dst.at[i], load_sem.at[kind, i])

    def load_probes(i):
        rows = pl.ds(i * 12, 12)
        return pltpu.make_async_copy(probes.at[rows], probes_v.at[rows], probe_sem.at[i])

    for i in range(8):
        load(0, i).start()
        load(1, i).start()
    for i in range(8):
        load_probes(i).start()
    for peer in peers:
        pl.semaphore_signal(barrier, 1, device_id=peer, device_id_type=MESH)

    def remote(src, dst, send, receive, target):
        return pltpu.make_async_remote_copy(
            src_ref=src, dst_ref=dst, send_sem=send, recv_sem=receive,
            device_id=target, device_id_type=MESH,
        )

    def plane_of(k):
        dy, dz = offset_of(k)
        return lax.rem(z - dz + 4, 4) * 4 + lax.rem(y - dy + 4, 4)

    def slot(plane, src_core, src_x):
        return plane * 8 + src_core * 4 + src_x

    def near(k):
        dy, dz = offset_of(k)
        return remote(staged.at[k, 0], recv.at[slot(mine, core, x)], near_s.at[k], near_r.at[k],
                      device(x, y + dy, z + dz, core))

    def far(k):
        dy, dz = offset_of(k)
        return remote(staged.at[k, 1], relay.at[k], far_s.at[k], far_r.at[k],
                      device(x, y + dy, z + dz, core))

    def along(k):
        own = recv.at[slot(plane_of(k), core, x)]
        return (
            remote(relay.at[k], own, x_s.at[k, 0], x_r.at[k, 0], device(x + 1, y, z, core)),
            remote(relay.at[k], own, x_s.at[k, 1], x_r.at[k, 1], device(x + 3, y, z, core)),
            remote(own, own, x_s.at[k, 2], x_r.at[k, 2], device(x + 2, y, z, core)),
        )

    def diagonal():
        k, own = ROUNDS - 1, recv.at[slot(mine, core, x)]
        return [
            remote(staged.at[k, other], own, x_s.at[k, i], x_r.at[k, i],
                   device(x + d, y + 2, z + 2, core))
            for i, (d, other) in enumerate(((1, 1), (3, 1), (2, 0)))
        ]

    def across(k):
        half = recv.at[pl.ds(slot(plane_of(k), core, 0), 4)]
        return remote(half, half, d_s.at[k], d_r.at[k], device(x, y, z, 1 - core))

    def piece(source, k, other, part):
        dy, dz = offset_of(k)
        low = lax.rem(x + other, 2)
        j = lax.rem(z + dz, 4) * 8 + low * 4 + lax.rem(y + dy, 4)
        return source[:, owner[j], part].reshape(64, 128).astype(BF16)

    def cut(dst, k, other):
        for row, source in ((0, query_f), (64, output_f)):
            for part in (0, 1):
                dst[row : row + 64, part * 128 : (part + 1) * 128] = piece(source, k, other, part)

    def stage(k):
        for other in (0, 1):
            cut(staged.at[k, other], k, other)

    for i in range(8):
        load(0, i).wait()
        load(1, i).wait()
    cut(recv.at[slot(mine, core, x)], 0, 0)
    cut(relay.at[0], 0, 1)
    if DIRECT:
        stage(ROUNDS - 1)
    stage(1)
    pl.semaphore_wait(barrier, len(peers))
    for copy in along(0):
        copy.start()
    far(1).start()
    near(1).start()
    if DIRECT:
        for copy in diagonal():
            copy.start()
    stage(2)

    @pl.loop(2, ROUNDS - DIRECT)
    def _(k):
        @pl.when(k < ROUNDS - 1 - DIRECT)
        def _():
            stage(k + 1)

        far(k).start()
        near(k).start()

    if DIRECT:
        near(ROUNDS - 1).start()

    prints[...] = jnp.zeros_like(prints)

    held_block = jnp.broadcast_to(block_row[...].astype(F32), (128, 128)).T
    shard = lax.broadcasted_iota(jnp.int32, (128, 128), 0)
    rep, tp = lax.div(shard, 32), lax.rem(shard, 32)
    src_x = lax.div(rep, 2) * 2 + lax.rem(lax.div(tp, 4), 2)
    where = slot(lax.div(tp, 8) * 4 + lax.rem(tp, 4), lax.rem(rep, 2), src_x)
    hit = held_block == lax.broadcasted_iota(jnp.int32, (128, 128), 1).astype(F32)
    slot_of[...] = jnp.sum(
        jnp.where(hit, where.astype(F32), 0.0), axis=0, keepdims=True
    ).astype(jnp.int32)

    half = lax.div(lax.broadcasted_iota(jnp.int32, (128, 256), 0), 64)

    def compute(k, src_core):
        plane = plane_of(k)
        src_z, src_y = lax.div(plane, 4), lax.rem(plane, 4)
        for src_x in range(4):
            shard = ((src_x // 2) * 2 + src_core) * 32 + src_z * 8 + (src_x % 2) * 4 + src_y
            at = block[shard]
            at_slot = slot(plane, src_core, src_x)
            lhs[:, src_x * 128 : (src_x + 1) * 128] = probes_v[:, lax.div(at, 2)].reshape(768, 128)
            q = recv[at_slot, 0:64, :]
            o = recv[at_slot, 64:128, :]
            held = half == lax.rem(at, 2)
            for part, data in enumerate((q, o)):
                pair = jnp.concatenate([data, data], axis=0)
                cols = slice(part * 256, (part + 1) * 256)
                rhs[src_x * 128 : (src_x + 1) * 128, cols] = jnp.where(
                    held, pair, jnp.zeros_like(pair)
                )
            turned[at_slot] = jnp.concatenate([o, o], axis=0).T

        @pl.loop(0, 3)
        def _(m):
            rows = pl.ds(pl.multiple_of(m * 256, 256), 256)
            prints[rows, :] += jnp.dot(lhs[rows, :], rhs[...], preferred_element_type=F32)

    @pl.loop(0, ROUNDS + LAG_D)
    def _(t):
        @pl.when((t >= 1) & (t < ROUNDS - DIRECT))
        def _():
            far(t).wait_recv()
            first, second, third = along(t)
            first.start()
            second.start()
            near(t).wait_recv()
            third.start()

        if DIRECT:
            @pl.when(t == ROUNDS - 1)
            def _():
                near(t).wait_recv()

        @pl.when((t >= LAG_X) & (t < ROUNDS + LAG_X))
        def _():
            for copy in along(t - LAG_X):
                copy.wait_recv()
            across(t - LAG_X).start()

            @pl.when(t == LAG_X)
            def _():
                for i in range(8):
                    load_probes(i).wait()

            compute(t - LAG_X, core)

        @pl.when(t >= LAG_D)
        def _():
            across(t - LAG_D).wait_recv()
            compute(t - LAG_D, 1 - core)

    @pl.loop(0, ROUNDS)
    def _(k):
        @pl.when(k >= 1)
        def _():
            near(k).wait_send()

        @pl.when((k >= 1) & (k < ROUNDS - DIRECT))
        def _():
            far(k).wait_send()

        for copy in along(k):
            copy.wait_send()
        across(k).wait_send()


def place_kernel(slot_of, recv, turned, prints, q_out, o_out, qp_out, op_out,
                 o_all, op_all, sems):
    qp = pltpu.make_async_copy(prints.at[:, 0:256], qp_out, sems.at[1])
    qp.start()
    left = lax.broadcasted_iota(jnp.int32, (256, 128), 1) < 64
    outs = []
    for part in range(4):
        @pl.loop(part * 16, (part + 1) * 16)
        def _(p):
            slots = slot_of[0, 2 * p], slot_of[0, 2 * p + 1]
            for i in (0, 1):
                rows = pl.ds(pl.multiple_of(p * 128 + i * 64, 64), 64)
                pltpu.make_async_copy(
                    recv.at[slots[i], 0:64, :], q_out.at[rows, :], sems.at[0]
                ).start()
            cols = pl.ds(pl.multiple_of(p * 128, 128), 128)
            o_all[:, cols] = jnp.where(left, turned[slots[0]], turned[slots[1]])

        cols = slice(part * 2048, (part + 1) * 2048)
        copy = pltpu.make_async_copy(o_all.at[:, cols], o_out.at[:, cols], sems.at[3 + part])
        copy.start()
        outs.append(copy)
    op_all[...] = prints[:, 256:512].T
    op = pltpu.make_async_copy(op_all, op_out, sems.at[2])
    op.start()
    for copy in [qp, op] + outs:
        copy.wait()
    pltpu.make_async_copy(q_out, q_out, sems.at[0]).wait()


def tiles(shard):
    return shard.reshape(8, 8, 32, 2, 128).transpose(0, 2, 3, 1, 4)


def per_device(trainer_query, trainer_output, probes, shard_block, slice_owner):
    smem = pl.BlockSpec(memory_space=pltpu.SMEM)
    hbm = pl.BlockSpec(memory_space=pltpu.HBM)
    vmem = pl.BlockSpec(memory_space=pltpu.VMEM)
    dma = pltpu.SemaphoreType.DMA

    def in_hbm(array):
        return pltpu.with_memory_space_constraint(array, pltpu.HBM)

    recv, turned, prints, slot_of = pl.pallas_call(
        move_kernel,
        out_shape=(
            pltpu.VMEM((128, 128, 256), BF16),
            pltpu.VMEM((128, 256, 128), BF16),
            pltpu.VMEM((768, 512), F32),
            pltpu.VMEM((1, 128), jnp.int32),
        ),
        in_specs=[smem, smem, vmem, hbm, hbm, hbm],
        out_specs=(vmem, vmem, vmem, vmem),
        scratch_shapes=[
            pltpu.VMEM((8, 32, 2, 8, 128), F32),
            pltpu.VMEM((8, 32, 2, 8, 128), F32),
            pltpu.VMEM((96, 64, 8, 128), BF16),
            pltpu.VMEM((ROUNDS, 2, 128, 256), BF16),
            pltpu.VMEM((ROUNDS, 128, 256), BF16),
            pltpu.VMEM((768, 512), BF16),
            pltpu.VMEM((512, 512), BF16),
            dma((2, 8)), dma((8,)), dma((ROUNDS,)), dma((ROUNDS,)), dma((ROUNDS,)), dma((ROUNDS,)),
            dma((ROUNDS, 3)), dma((ROUNDS, 3)), dma((ROUNDS,)), dma((ROUNDS,)),
        ],
        compiler_params=pltpu.CompilerParams(
            collective_id=0, has_side_effects=True, vmem_limit_bytes=30 << 20
        ),
        name="move",
    )(
        in_hbm(slice_owner),
        in_hbm(shard_block),
        in_hbm(shard_block.reshape(1, 128)),
        in_hbm(tiles(trainer_query[0])),
        in_hbm(tiles(jnp.swapaxes(trainer_output, 1, 2)[0])),
        in_hbm(probes.reshape(96, 8, 64, 128).transpose(0, 2, 1, 3)),
    )
    outs = pl.pallas_call(
        place_kernel,
        out_shape=(
            jax.ShapeDtypeStruct((8192, 256), BF16),
            jax.ShapeDtypeStruct((256, 8192), BF16),
            jax.ShapeDtypeStruct((768, 256), F32),
            jax.ShapeDtypeStruct((256, 768), F32),
        ),
        in_specs=[smem, vmem, vmem, vmem],
        out_specs=(hbm, hbm, hbm, hbm),
        scratch_shapes=[
            pltpu.VMEM((256, 8192), BF16),
            pltpu.VMEM((256, 768), F32),
            dma((8,)),
        ],
        compiler_params=pltpu.CompilerParams(vmem_limit_bytes=10 << 20),
        name="place",
    )(slot_of, recv, turned, prints)
    return tuple(out[None] for out in outs)


def solution(mesh):
    placed = (P(("rep", "tp"), None, None), P(("rep", "tp"), None, None), P(), P(), P())
    return jax.shard_map(
        per_device,
        mesh=mesh,
        in_specs=placed,
        out_specs=(
            P("tp", None, None),
            P("tp", None, None),
            P("tp", None, None),
            P("tp", None, None),
        ),
        check_vma=False,
    )
```

```python
import jax
import jax.numpy as jnp
from jax import lax
from jax.experimental import pallas as pl
from jax.experimental.pallas import tpu as pltpu
from jax.sharding import PartitionSpec as P

MESH = pl.DeviceIdType.MESH
BF16 = jnp.bfloat16
F32 = jnp.float32

ROUNDS = 16
LAG_X = 3
LAG_D = 4
DIRECT = 0
AHEAD = 4


def near_first(i):
    return lax.rem(lax.div(i * (i + 1), 2), 4)


def offset_of(k):
    k = jnp.int32(k)
    return near_first(lax.rem(k, 4)), near_first(lax.div(k, 4))


def place():
    rep, tp = lax.axis_index("rep"), lax.axis_index("tp")
    x = lax.div(rep, 2) * 2 + lax.rem(lax.div(tp, 4), 2)
    return x, lax.rem(tp, 4), lax.div(tp, 8), lax.rem(rep, 2)


def device(x, y, z, core):
    x, y, z = lax.rem(x, 4), lax.rem(y, 4), lax.rem(z, 4)
    return {"rep": lax.div(x, 2) * 2 + core, "tp": z * 8 + lax.rem(x, 2) * 4 + y}


def move_kernel(
    owner, block, block_row, query, output, probes,
    recv, turned, prints, slot_of,
    query_f, output_f, probes_v, staged, relay, lhs, rhs,
    load_sem, probe_sem, near_s, near_r, far_s, far_r, x_s, x_r, d_s, d_r,
):
    x, y, z, core = place()
    mine = z * 4 + y
    barrier = pltpu.get_barrier_semaphore()
    peers = [device(x, y + k % 4, z + k // 4, core) for k in range(1, ROUNDS)]
    peers += [device(x + d, y, z, core) for d in (1, 2, 3)] + [device(x, y, z, 1 - core)]
    if DIRECT:
        peers += [device(x + d, y + 2, z + 2, core) for d in (1, 2, 3)]

    def load(kind, i):
        src, dst = ((query, query_f), (output, output_f))[kind]
        return pltpu.make_async_copy(src.at[i], dst.at[i], load_sem.at[kind, i])

    def load_probes(i):
        rows = pl.ds(i * 12, 12)
        return pltpu.make_async_copy(probes.at[rows], probes_v.at[rows], probe_sem.at[i])

    for i in range(8):
        load(0, i).start()
        load(1, i).start()
    for peer in peers:
        pl.semaphore_signal(barrier, 1, device_id=peer, device_id_type=MESH)

    def remote(src, dst, send, receive, target):
        return pltpu.make_async_remote_copy(
            src_ref=src, dst_ref=dst, send_sem=send, recv_sem=receive,
            device_id=target, device_id_type=MESH,
        )

    def plane_of(k):
        dy, dz = offset_of(k)
        return lax.rem(z - dz + 4, 4) * 4 + lax.rem(y - dy + 4, 4)

    def slot(plane, src_core, src_x):
        return plane * 8 + src_core * 4 + src_x

    def near(k):
        dy, dz = offset_of(k)
        return remote(staged.at[k, 0], recv.at[slot(mine, core, x)], near_s.at[k], near_r.at[k],
                      device(x, y + dy, z + dz, core))

    def far(k):
        dy, dz = offset_of(k)
        return remote(staged.at[k, 1], relay.at[k], far_s.at[k], far_r.at[k],
                      device(x, y + dy, z + dz, core))

    def along(k):
        own = recv.at[slot(plane_of(k), core, x)]
        return (
            remote(relay.at[k], own, x_s.at[k, 0], x_r.at[k, 0], device(x + 1, y, z, core)),
            remote(relay.at[k], own, x_s.at[k, 1], x_r.at[k, 1], device(x + 3, y, z, core)),
            remote(own, own, x_s.at[k, 2], x_r.at[k, 2], device(x + 2, y, z, core)),
        )

    def diagonal():
        k, own = ROUNDS - 1, recv.at[slot(mine, core, x)]
        return [
            remote(staged.at[k, other], own, x_s.at[k, i], x_r.at[k, i],
                   device(x + d, y + 2, z + 2, core))
            for i, (d, other) in enumerate(((1, 1), (3, 1), (2, 0)))
        ]

    def across(k):
        half = recv.at[pl.ds(slot(plane_of(k), core, 0), 4)]
        return remote(half, half, d_s.at[k], d_r.at[k], device(x, y, z, 1 - core))

    def piece(source, k, other, part):
        dy, dz = offset_of(k)
        low = lax.rem(x + other, 2)
        j = lax.rem(z + dz, 4) * 8 + low * 4 + lax.rem(y + dy, 4)
        return source[:, owner[j], part].reshape(64, 128).astype(BF16)

    def cut(dst, k, other):
        for row, source in ((0, query_f), (64, output_f)):
            for part in (0, 1):
                dst[row : row + 64, part * 128 : (part + 1) * 128] = piece(source, k, other, part)

    def stage(k):
        for other in (0, 1):
            cut(staged.at[k, other], k, other)

    for i in range(8):
        load(0, i).wait()
        load(1, i).wait()
    cut(recv.at[slot(mine, core, x)], 0, 0)
    cut(relay.at[0], 0, 1)
    if DIRECT:
        stage(ROUNDS - 1)
    stage(1)
    pl.semaphore_wait(barrier, len(peers))
    for copy in along(0):
        copy.start()
    far(1).start()
    near(1).start()
    if DIRECT:
        for copy in diagonal():
            copy.start()
    for k in range(2, AHEAD + 1):
        stage(k)
        far(k).start()
        near(k).start()

    for i in range(8):
        load_probes(i).start()
    prints[...] = jnp.zeros_like(prints)

    held_block = jnp.broadcast_to(block_row[...].astype(F32), (128, 128)).T
    shard = lax.broadcasted_iota(jnp.int32, (128, 128), 0)
    rep, tp = lax.div(shard, 32), lax.rem(shard, 32)
    src_x = lax.div(rep, 2) * 2 + lax.rem(lax.div(tp, 4), 2)
    where = slot(lax.div(tp, 8) * 4 + lax.rem(tp, 4), lax.rem(rep, 2), src_x)
    hit = held_block == lax.broadcasted_iota(jnp.int32, (128, 128), 1).astype(F32)
    slot_of[...] = jnp.sum(
        jnp.where(hit, where.astype(F32), 0.0), axis=0, keepdims=True
    ).astype(jnp.int32)

    half = lax.div(lax.broadcasted_iota(jnp.int32, (128, 256), 0), 64)

    lane_half = lax.div(lax.broadcasted_iota(jnp.int32, (768, 128), 1), 64)

    def arrange(k, src_core, at_half):
        plane = plane_of(k)
        src_z, src_y = lax.div(plane, 4), lax.rem(plane, 4)
        for pair in range(2):
            ats, qs, os = [], [], []
            for src_x in (2 * pair, 2 * pair + 1):
                shard = ((src_x // 2) * 2 + src_core) * 32 + src_z * 8 + (src_x % 2) * 4 + src_y
                at_slot = slot(plane, src_core, src_x)
                q, o = recv[at_slot, 0:64, :], recv[at_slot, 64:128, :]
                q, o = (jnp.concatenate([part, part], axis=0) for part in (q, o))
                turned[at_slot] = o.T
                ats.append(block[shard])
                qs.append(q)
                os.append(o)
            side = lax.rem(ats[0], 2)
            one, two = (probes_v[:, lax.div(at, 2)].reshape(768, 128) for at in ats)
            swapped = pltpu.roll(two, 64, axis=1)
            two = jnp.where(lane_half * 0 + side == lax.rem(ats[1], 2), swapped, two)
            rows = slice(at_half * 256 + pair * 128, at_half * 256 + (pair + 1) * 128)
            lhs[:, rows] = jnp.where(lane_half == side, one, two)
            rhs[rows, 0:256] = jnp.where(half == side, *qs)
            rhs[rows, 256:512] = jnp.where(half == side, *os)

    def accumulate():
        @pl.loop(0, 3)
        def _(m):
            rows = pl.ds(pl.multiple_of(m * 256, 256), 256)
            prints[rows, :] += jnp.dot(lhs[rows, :], rhs[...], preferred_element_type=F32)

    @pl.loop(0, ROUNDS + LAG_D)
    def _(t):
        @pl.when((t >= 1) & (t + AHEAD < ROUNDS))
        def _():
            stage(t + AHEAD)
            far(t + AHEAD).start()
            near(t + AHEAD).start()

        @pl.when((t >= 1) & (t < ROUNDS - DIRECT))
        def _():
            far(t).wait_recv()
            first, second, third = along(t)
            first.start()
            second.start()
            near(t).wait_recv()
            third.start()

        if DIRECT:
            @pl.when(t == ROUNDS - 1)
            def _():
                near(t).wait_recv()

        @pl.when((t >= LAG_X) & (t < ROUNDS + LAG_X))
        def _():
            for copy in along(t - LAG_X):
                copy.wait_recv()
            across(t - LAG_X).start()

            @pl.when(t == LAG_X)
            def _():
                for i in range(8):
                    load_probes(i).wait()

        @pl.when(t >= LAG_D)
        def _():
            across(t - LAG_D).wait_recv()
            arrange(t - LAG_D, 1 - core, 1)
            accumulate()

        @pl.when((t >= LAG_X) & (t < ROUNDS + LAG_X))
        def _():
            arrange(t - LAG_X, core, 0)

    @pl.loop(0, ROUNDS)
    def _(k):
        @pl.when(k >= 1)
        def _():
            near(k).wait_send()

        @pl.when((k >= 1) & (k < ROUNDS - DIRECT))
        def _():
            far(k).wait_send()

        for copy in along(k):
            copy.wait_send()
        across(k).wait_send()


def place_kernel(slot_of, recv, turned, prints, q_out, o_out, qp_out, op_out,
                 o_all, op_all, sems):
    qp = pltpu.make_async_copy(prints.at[:, 0:256], qp_out, sems.at[1])
    qp.start()
    left = lax.broadcasted_iota(jnp.int32, (256, 128), 1) < 64
    outs = []
    for part in range(4):
        @pl.loop(part * 16, (part + 1) * 16)
        def _(p):
            slots = slot_of[0, 2 * p], slot_of[0, 2 * p + 1]
            for i in (0, 1):
                rows = pl.ds(pl.multiple_of(p * 128 + i * 64, 64), 64)
                pltpu.make_async_copy(
                    recv.at[slots[i], 0:64, :], q_out.at[rows, :], sems.at[0]
                ).start()
            cols = pl.ds(pl.multiple_of(p * 128, 128), 128)
            o_all[:, cols] = jnp.where(left, turned[slots[0]], turned[slots[1]])

        cols = slice(part * 2048, (part + 1) * 2048)
        copy = pltpu.make_async_copy(o_all.at[:, cols], o_out.at[:, cols], sems.at[3 + part])
        copy.start()
        outs.append(copy)
    op_all[...] = prints[:, 256:512].T
    op = pltpu.make_async_copy(op_all, op_out, sems.at[2])
    op.start()
    for copy in [qp, op] + outs:
        copy.wait()
    pltpu.make_async_copy(q_out, q_out, sems.at[0]).wait()


def tiles(shard):
    return shard.reshape(8, 8, 32, 2, 128).transpose(0, 2, 3, 1, 4)


def per_device(trainer_query, trainer_output, probes, shard_block, slice_owner):
    smem = pl.BlockSpec(memory_space=pltpu.SMEM)
    hbm = pl.BlockSpec(memory_space=pltpu.HBM)
    vmem = pl.BlockSpec(memory_space=pltpu.VMEM)
    dma = pltpu.SemaphoreType.DMA

    def in_hbm(array):
        return pltpu.with_memory_space_constraint(array, pltpu.HBM)

    recv, turned, prints, slot_of = pl.pallas_call(
        move_kernel,
        out_shape=(
            pltpu.VMEM((128, 128, 256), BF16),
            pltpu.VMEM((128, 256, 128), BF16),
            pltpu.VMEM((768, 512), F32),
            pltpu.VMEM((1, 128), jnp.int32),
        ),
        in_specs=[smem, smem, vmem, hbm, hbm, hbm],
        out_specs=(vmem, vmem, vmem, vmem),
        scratch_shapes=[
            pltpu.VMEM((8, 32, 2, 8, 128), F32),
            pltpu.VMEM((8, 32, 2, 8, 128), F32),
            pltpu.VMEM((96, 64, 8, 128), BF16),
            pltpu.VMEM((ROUNDS, 2, 128, 256), BF16),
            pltpu.VMEM((ROUNDS, 128, 256), BF16),
            pltpu.VMEM((768, 512), BF16),
            pltpu.VMEM((512, 512), BF16),
            dma((2, 8)), dma((8,)), dma((ROUNDS,)), dma((ROUNDS,)), dma((ROUNDS,)), dma((ROUNDS,)),
            dma((ROUNDS, 3)), dma((ROUNDS, 3)), dma((ROUNDS,)), dma((ROUNDS,)),
        ],
        compiler_params=pltpu.CompilerParams(
            collective_id=0, has_side_effects=True, vmem_limit_bytes=30 << 20
        ),
        name="move",
    )(
        in_hbm(slice_owner),
        in_hbm(shard_block),
        in_hbm(shard_block.reshape(1, 128)),
        in_hbm(tiles(trainer_query[0])),
        in_hbm(tiles(jnp.swapaxes(trainer_output, 1, 2)[0])),
        in_hbm(probes.reshape(96, 8, 64, 128).transpose(0, 2, 1, 3)),
    )
    outs = pl.pallas_call(
        place_kernel,
        out_shape=(
            jax.ShapeDtypeStruct((8192, 256), BF16),
            jax.ShapeDtypeStruct((256, 8192), BF16),
            jax.ShapeDtypeStruct((768, 256), F32),
            jax.ShapeDtypeStruct((256, 768), F32),
        ),
        in_specs=[smem, vmem, vmem, vmem],
        out_specs=(hbm, hbm, hbm, hbm),
        scratch_shapes=[
            pltpu.VMEM((256, 8192), BF16),
            pltpu.VMEM((256, 768), F32),
            dma((8,)),
        ],
        compiler_params=pltpu.CompilerParams(vmem_limit_bytes=10 << 20),
        name="place",
    )(slot_of, recv, turned, prints)
    return tuple(out[None] for out in outs)


def solution(mesh):
    placed = (P(("rep", "tp"), None, None), P(("rep", "tp"), None, None), P(), P(), P())
    return jax.shard_map(
        per_device,
        mesh=mesh,
        in_specs=placed,
        out_specs=(
            P("tp", None, None),
            P("tp", None, None),
            P("tp", None, None),
            P("tp", None, None),
        ),
        check_vma=False,
    )
```

```python
import jax
import jax.numpy as jnp
from jax import lax
from jax.experimental import pallas as pl
from jax.experimental.pallas import tpu as pltpu
from jax.sharding import PartitionSpec as P

MESH = pl.DeviceIdType.MESH
BF16 = jnp.bfloat16
F32 = jnp.float32

ROUNDS = 16
LAG_X = 3
LAG_D = 4
AHEAD = 4


def near_first(i):
    return lax.rem(lax.div(i * (i + 1), 2), 4)


def offset_of(k):
    k = jnp.int32(k)
    return near_first(lax.rem(k, 4)), near_first(lax.div(k, 4))


def place():
    rep, tp = lax.axis_index("rep"), lax.axis_index("tp")
    x = lax.div(rep, 2) * 2 + lax.rem(lax.div(tp, 4), 2)
    return x, lax.rem(tp, 4), lax.div(tp, 8), lax.rem(rep, 2)


def device(x, y, z, core):
    x, y, z = lax.rem(x, 4), lax.rem(y, 4), lax.rem(z, 4)
    return {"rep": lax.div(x, 2) * 2 + core, "tp": z * 8 + lax.rem(x, 2) * 4 + y}


def move_kernel(
    owner_hbm, block_hbm, query, output, probes,
    recv, turned, prints, slot_of,
    owner, block, block_row, slot_row, query_f, output_f, probes_v, staged, relay, lhs, rhs,
    level, map_sem, load_sem, probe_sem, near_s, near_r, far_s, far_r, x_s, x_r, d_s, d_r,
):
    x, y, z, core = place()
    mine = z * 4 + y
    barrier = pltpu.get_barrier_semaphore()
    beside = [device(x, y + dy, z + dz, core) for dy, dz in ((1, 0), (3, 0), (0, 1), (0, 3))]
    peers = [device(x + d, y, z, core) for d in (1, 2, 3)] + [device(x, y, z, 1 - core)] + beside

    def load(kind, i):
        src, dst = ((query, query_f), (output, output_f))[kind]
        return pltpu.make_async_copy(src.at[i], dst.at[i], load_sem.at[kind, i])

    def load_probes(i):
        rows = pl.ds(i * 12, 12)
        return pltpu.make_async_copy(probes.at[rows], probes_v.at[rows], probe_sem.at[i])

    maps = [
        pltpu.make_async_copy(owner_hbm, owner, map_sem.at[0]),
        pltpu.make_async_copy(block_hbm, block, map_sem.at[1]),
        pltpu.make_async_copy(block_hbm, block_row, map_sem.at[2]),
    ]
    for copy in maps:
        copy.start()
    for i in range(8):
        load(0, i).start()
        load(1, i).start()
    for peer in peers:
        pl.semaphore_signal(barrier, 1, device_id=peer, device_id_type=MESH)

    def remote(src, dst, send, receive, target):
        return pltpu.make_async_remote_copy(
            src_ref=src, dst_ref=dst, send_sem=send, recv_sem=receive,
            device_id=target, device_id_type=MESH,
        )

    def plane_of(k):
        dy, dz = offset_of(k)
        return lax.rem(z - dz + 4, 4) * 4 + lax.rem(y - dy + 4, 4)

    def slot(plane, src_core, src_x):
        return plane * 8 + src_core * 4 + src_x

    def near(k):
        dy, dz = offset_of(k)
        return remote(staged.at[k, 0], recv.at[slot(mine, core, x)], near_s.at[k], near_r.at[k],
                      device(x, y + dy, z + dz, core))

    def far(k):
        dy, dz = offset_of(k)
        return remote(staged.at[k, 1], relay.at[k], far_s.at[k], far_r.at[k],
                      device(x, y + dy, z + dz, core))

    def along(k):
        own = recv.at[slot(plane_of(k), core, x)]
        return (
            remote(relay.at[k], own, x_s.at[k, 0], x_r.at[k, 0], device(x + 1, y, z, core)),
            remote(relay.at[k], own, x_s.at[k, 1], x_r.at[k, 1], device(x + 3, y, z, core)),
            remote(own, own, x_s.at[k, 2], x_r.at[k, 2], device(x + 2, y, z, core)),
        )

    def across(k):
        half = recv.at[pl.ds(slot(plane_of(k), core, 0), 4)]
        return remote(half, half, d_s.at[k], d_r.at[k], device(x, y, z, 1 - core))

    def piece(source, k, other, part):
        dy, dz = offset_of(k)
        low = lax.rem(x + other, 2)
        j = lax.rem(z + dz, 4) * 8 + low * 4 + lax.rem(y + dy, 4)
        return source[:, owner[j], part].reshape(64, 128).astype(BF16)

    def cut(dst, k, other):
        for row, source in ((0, query_f), (64, output_f)):
            for part in (0, 1):
                dst[row : row + 64, part * 128 : (part + 1) * 128] = piece(source, k, other, part)

    def stage(k):
        for other in (0, 1):
            cut(staged.at[k, other], k, other)

    def send(k):
        far(k).start()
        near(k).start()

    def pass_on(i):
        for peer in beside:
            pl.semaphore_signal(level.at[i], 1, device_id=peer, device_id_type=MESH)

    for copy in maps:
        copy.wait()
    for i in range(8):
        load(0, i).wait()
        load(1, i).wait()
    cut(recv.at[slot(mine, core, x)], 0, 0)
    cut(relay.at[0], 0, 1)
    stage(1)
    pl.semaphore_wait(barrier, len(peers))
    for copy in along(0):
        copy.start()
    send(1)
    pass_on(0)
    stage(2)
    send(2)
    stage(4)
    send(4)
    stage(3)
    pl.semaphore_wait(level.at[0], 4)
    pass_on(1)
    send(3)
    for i in range(8):
        load_probes(i).start()
    prints[...] = jnp.zeros_like(prints)

    held_block = jnp.broadcast_to(block_row[...].astype(F32), (128, 128)).T
    shard = lax.broadcasted_iota(jnp.int32, (128, 128), 0)
    rep, tp = lax.div(shard, 32), lax.rem(shard, 32)
    src_x = lax.div(rep, 2) * 2 + lax.rem(lax.div(tp, 4), 2)
    where = slot(lax.div(tp, 8) * 4 + lax.rem(tp, 4), lax.rem(rep, 2), src_x)
    hit = held_block == lax.broadcasted_iota(jnp.int32, (128, 128), 1).astype(F32)
    slot_row[...] = jnp.sum(
        jnp.where(hit, where.astype(F32), 0.0), axis=0, keepdims=True
    ).astype(jnp.int32)
    to_scalar = pltpu.make_async_copy(slot_row, slot_of, map_sem.at[0])
    to_scalar.start()

    half = lax.div(lax.broadcasted_iota(jnp.int32, (128, 256), 0), 64)

    lane_half = lax.div(lax.broadcasted_iota(jnp.int32, (768, 128), 1), 64)

    def arrange(k, src_core, at_half):
        plane = plane_of(k)
        src_z, src_y = lax.div(plane, 4), lax.rem(plane, 4)
        for pair in range(2):
            ats, qs, os = [], [], []
            for src_x in (2 * pair, 2 * pair + 1):
                shard = ((src_x // 2) * 2 + src_core) * 32 + src_z * 8 + (src_x % 2) * 4 + src_y
                at_slot = slot(plane, src_core, src_x)
                q, o = recv[at_slot, 0:64, :], recv[at_slot, 64:128, :]
                q, o = (jnp.concatenate([part, part], axis=0) for part in (q, o))
                turned[at_slot] = o.T
                ats.append(block[0, shard])
                qs.append(q)
                os.append(o)
            side = lax.rem(ats[0], 2)
            one, two = (probes_v[:, lax.div(at, 2)].reshape(768, 128) for at in ats)
            swapped = pltpu.roll(two, 64, axis=1)
            two = jnp.where(lane_half * 0 + side == lax.rem(ats[1], 2), swapped, two)
            rows = slice(at_half * 256 + pair * 128, at_half * 256 + (pair + 1) * 128)
            lhs[:, rows] = jnp.where(lane_half == side, one, two)
            rhs[rows, 0:256] = jnp.where(half == side, *qs)
            rhs[rows, 256:512] = jnp.where(half == side, *os)

    def accumulate():
        @pl.loop(0, 3)
        def _(m):
            rows = pl.ds(pl.multiple_of(m * 256, 256), 256)
            prints[rows, :] += jnp.dot(lhs[rows, :], rhs[...], preferred_element_type=F32)

    @pl.loop(0, ROUNDS + LAG_D)
    def _(t):
        @pl.when((t >= 1) & (t + AHEAD < ROUNDS))
        def _():
            stage(t + AHEAD)

            @pl.when(t + AHEAD == 7)
            def _():
                pl.semaphore_wait(level.at[1], 4)
                pass_on(2)

            @pl.when(t + AHEAD == 15)
            def _():
                pl.semaphore_wait(level.at[2], 4)

            send(t + AHEAD)

        @pl.when((t >= 1) & (t < ROUNDS))
        def _():
            far(t).wait_recv()
            first, second, third = along(t)
            first.start()
            second.start()
            near(t).wait_recv()
            third.start()

        @pl.when((t >= LAG_X) & (t < ROUNDS + LAG_X))
        def _():
            for copy in along(t - LAG_X):
                copy.wait_recv()
            across(t - LAG_X).start()

            @pl.when(t == LAG_X)
            def _():
                for i in range(8):
                    load_probes(i).wait()

        @pl.when(t >= LAG_D)
        def _():
            across(t - LAG_D).wait_recv()
            arrange(t - LAG_D, 1 - core, 1)
            accumulate()

        @pl.when((t >= LAG_X) & (t < ROUNDS + LAG_X))
        def _():
            arrange(t - LAG_X, core, 0)

    to_scalar.wait()

    @pl.loop(0, ROUNDS)
    def _(k):
        @pl.when(k >= 1)
        def _():
            near(k).wait_send()
            far(k).wait_send()

        for copy in along(k):
            copy.wait_send()
        across(k).wait_send()


def place_kernel(slot_of, recv, turned, prints, q_out, o_out, qp_out, op_out,
                 o_all, op_all, sems):
    qp = pltpu.make_async_copy(prints.at[:, 0:256], qp_out, sems.at[1])
    qp.start()
    left = lax.broadcasted_iota(jnp.int32, (256, 128), 1) < 64
    outs = []
    for part in range(4):
        @pl.loop(part * 16, (part + 1) * 16)
        def _(p):
            slots = slot_of[0, 2 * p], slot_of[0, 2 * p + 1]
            for i in (0, 1):
                rows = pl.ds(pl.multiple_of(p * 128 + i * 64, 64), 64)
                pltpu.make_async_copy(
                    recv.at[slots[i], 0:64, :], q_out.at[rows, :], sems.at[0]
                ).start()
            cols = pl.ds(pl.multiple_of(p * 128, 128), 128)
            o_all[:, cols] = jnp.where(left, turned[slots[0]], turned[slots[1]])

        cols = slice(part * 2048, (part + 1) * 2048)
        copy = pltpu.make_async_copy(o_all.at[:, cols], o_out.at[:, cols], sems.at[3 + part])
        copy.start()
        outs.append(copy)
    op_all[...] = prints[:, 256:512].T
    op = pltpu.make_async_copy(op_all, op_out, sems.at[2])
    op.start()
    for copy in [qp, op] + outs:
        copy.wait()
    pltpu.make_async_copy(q_out, q_out, sems.at[0]).wait()


def tiles(shard):
    return shard.reshape(8, 8, 32, 2, 128).transpose(0, 2, 3, 1, 4)


def per_device(trainer_query, trainer_output, probes, shard_block, slice_owner):
    smem = pl.BlockSpec(memory_space=pltpu.SMEM)
    hbm = pl.BlockSpec(memory_space=pltpu.HBM)
    vmem = pl.BlockSpec(memory_space=pltpu.VMEM)
    dma = pltpu.SemaphoreType.DMA

    def in_hbm(array):
        return pltpu.with_memory_space_constraint(array, pltpu.HBM)

    recv, turned, prints, slot_of = pl.pallas_call(
        move_kernel,
        out_shape=(
            pltpu.VMEM((128, 128, 256), BF16),
            pltpu.VMEM((128, 256, 128), BF16),
            pltpu.VMEM((768, 512), F32),
            pltpu.SMEM((1, 128), jnp.int32),
        ),
        in_specs=[hbm, hbm, hbm, hbm, hbm],
        out_specs=(vmem, vmem, vmem, smem),
        scratch_shapes=[
            pltpu.SMEM((32,), jnp.int32),
            pltpu.SMEM((1, 128), jnp.int32),
            pltpu.VMEM((1, 128), jnp.int32),
            pltpu.VMEM((1, 128), jnp.int32),
            pltpu.VMEM((8, 32, 2, 8, 128), F32),
            pltpu.VMEM((8, 32, 2, 8, 128), F32),
            pltpu.VMEM((96, 64, 8, 128), BF16),
            pltpu.VMEM((ROUNDS, 2, 128, 256), BF16),
            pltpu.VMEM((ROUNDS, 128, 256), BF16),
            pltpu.VMEM((768, 512), BF16),
            pltpu.VMEM((512, 512), BF16),
            pltpu.SemaphoreType.REGULAR((3,)), dma((3,)), dma((2, 8)), dma((8,)), dma((ROUNDS,)), dma((ROUNDS,)), dma((ROUNDS,)), dma((ROUNDS,)),
            dma((ROUNDS, 3)), dma((ROUNDS, 3)), dma((ROUNDS,)), dma((ROUNDS,)),
        ],
        compiler_params=pltpu.CompilerParams(
            collective_id=0, has_side_effects=True, vmem_limit_bytes=30 << 20
        ),
        name="move",
    )(
        in_hbm(slice_owner),
        in_hbm(shard_block.reshape(1, 128)),
        in_hbm(tiles(trainer_query[0])),
        in_hbm(tiles(jnp.swapaxes(trainer_output, 1, 2)[0])),
        in_hbm(probes.reshape(96, 8, 64, 128).transpose(0, 2, 1, 3)),
    )
    outs = pl.pallas_call(
        place_kernel,
        out_shape=(
            jax.ShapeDtypeStruct((8192, 256), BF16),
            jax.ShapeDtypeStruct((256, 8192), BF16),
            jax.ShapeDtypeStruct((768, 256), F32),
            jax.ShapeDtypeStruct((256, 768), F32),
        ),
        in_specs=[smem, vmem, vmem, vmem],
        out_specs=(hbm, hbm, hbm, hbm),
        scratch_shapes=[
            pltpu.VMEM((256, 8192), BF16),
            pltpu.VMEM((256, 768), F32),
            dma((8,)),
        ],
        compiler_params=pltpu.CompilerParams(vmem_limit_bytes=10 << 20),
        name="place",
    )(slot_of, recv, turned, prints)
    return tuple(out[None] for out in outs)


def solution(mesh):
    placed = (P(("rep", "tp"), None, None), P(("rep", "tp"), None, None), P(), P(), P())
    return jax.shard_map(
        per_device,
        mesh=mesh,
        in_specs=placed,
        out_specs=(
            P("tp", None, None),
            P("tp", None, None),
            P("tp", None, None),
            P("tp", None, None),
        ),
        check_vma=False,
    )
```

```python
import jax
import jax.numpy as jnp
from jax import lax
from jax.experimental import pallas as pl
from jax.experimental.pallas import tpu as pltpu
from jax.sharding import PartitionSpec as P

MESH = pl.DeviceIdType.MESH
BF16 = jnp.bfloat16
F32 = jnp.float32

ROUNDS = 16
LAG_X = 3
LAG_D = 4
AHEAD = 6


STEPS = (
    (0, 0), (1, 0), (0, 1), (3, 0), (0, 3), (1, 1), (3, 3), (2, 0),
    (1, 3), (3, 1), (0, 2), (2, 1), (1, 2), (2, 3), (3, 2), (2, 2),
)


def offset_of(k):
    k = jnp.int32(k)
    return tuple(
        sum(steps[i] * (k == n).astype(jnp.int32) for n, steps in enumerate(STEPS) if steps[i])
        for i in (0, 1)
    )


def place():
    rep, tp = lax.axis_index("rep"), lax.axis_index("tp")
    x = lax.div(rep, 2) * 2 + lax.rem(lax.div(tp, 4), 2)
    return x, lax.rem(tp, 4), lax.div(tp, 8), lax.rem(rep, 2)


def device(x, y, z, core):
    x, y, z = lax.rem(x, 4), lax.rem(y, 4), lax.rem(z, 4)
    return {"rep": lax.div(x, 2) * 2 + core, "tp": z * 8 + lax.rem(x, 2) * 4 + y}


def move_kernel(
    owner_hbm, block_hbm, query, output, probes,
    recv, turned, prints, slot_of,
    owner, block, block_row, slot_row, query_f, output_f, probes_v, staged, relay, lhs, rhs,
    level, map_sem, load_sem, probe_sem, near_s, near_r, far_s, far_r, x_s, x_r, d_s, d_r,
):
    x, y, z, core = place()
    mine = z * 4 + y
    barrier = pltpu.get_barrier_semaphore()
    beside = [device(x, y + dy, z + dz, core) for dy, dz in ((1, 0), (3, 0), (0, 1), (0, 3))]
    peers = [device(x + d, y, z, core) for d in (1, 2, 3)] + [device(x, y, z, 1 - core)] + beside

    for peer in peers:
        pl.semaphore_signal(barrier, 1, device_id=peer, device_id_type=MESH)

    def load(kind, i):
        src, dst = ((query, query_f), (output, output_f))[kind]
        return pltpu.make_async_copy(src.at[i], dst.at[i], load_sem.at[kind, i])

    def load_probes(i):
        rows = pl.ds(i * 12, 12)
        return pltpu.make_async_copy(probes.at[rows], probes_v.at[rows], probe_sem.at[i])

    maps = [
        pltpu.make_async_copy(owner_hbm, owner, map_sem.at[0]),
        pltpu.make_async_copy(block_hbm, block, map_sem.at[1]),
        pltpu.make_async_copy(block_hbm, block_row, map_sem.at[2]),
    ]
    for copy in maps:
        copy.start()
    for i in range(8):
        load(0, i).start()
        load(1, i).start()
    def remote(src, dst, send, receive, target):
        return pltpu.make_async_remote_copy(
            src_ref=src, dst_ref=dst, send_sem=send, recv_sem=receive,
            device_id=target, device_id_type=MESH,
        )

    def plane_of(k):
        dy, dz = offset_of(k)
        return lax.rem(z - dz + 4, 4) * 4 + lax.rem(y - dy + 4, 4)

    def slot(plane, src_core, src_x):
        return plane * 8 + src_core * 4 + src_x

    def near(k):
        dy, dz = offset_of(k)
        return remote(staged.at[k, 0], recv.at[slot(mine, core, x)], near_s.at[k], near_r.at[k],
                      device(x, y + dy, z + dz, core))

    def far(k):
        dy, dz = offset_of(k)
        return remote(staged.at[k, 1], relay.at[k], far_s.at[k], far_r.at[k],
                      device(x, y + dy, z + dz, core))

    def along(k):
        own = recv.at[slot(plane_of(k), core, x)]
        return (
            remote(relay.at[k], own, x_s.at[k, 0], x_r.at[k, 0], device(x + 1, y, z, core)),
            remote(relay.at[k], own, x_s.at[k, 1], x_r.at[k, 1], device(x + 3, y, z, core)),
            remote(own, own, x_s.at[k, 2], x_r.at[k, 2], device(x + 2, y, z, core)),
        )

    def across(k):
        half = recv.at[pl.ds(slot(plane_of(k), core, 0), 4)]
        return remote(half, half, d_s.at[k], d_r.at[k], device(x, y, z, 1 - core))

    def piece(source, k, other, part):
        dy, dz = offset_of(k)
        low = lax.rem(x + other, 2)
        j = lax.rem(z + dz, 4) * 8 + low * 4 + lax.rem(y + dy, 4)
        return source[:, owner[j], part].reshape(64, 128).astype(BF16)

    def cut(dst, k, other):
        for row, source in ((0, query_f), (64, output_f)):
            for part in (0, 1):
                dst[row : row + 64, part * 128 : (part + 1) * 128] = piece(source, k, other, part)

    def stage(k):
        for other in (0, 1):
            cut(staged.at[k, other], k, other)

    def send(k):
        far(k).start()
        near(k).start()

    def pass_on(i):
        for peer in beside:
            pl.semaphore_signal(level.at[i], 1, device_id=peer, device_id_type=MESH)

    for copy in maps:
        copy.wait()
    for i in range(8):
        load(0, i).wait()
        load(1, i).wait()
    cut(recv.at[slot(mine, core, x)], 0, 0)
    cut(relay.at[0], 0, 1)
    stage(1)
    pl.semaphore_wait(barrier, len(peers))
    for copy in along(0):
        copy.start()
    send(1)
    pass_on(0)
    for k in range(2, AHEAD + 1):
        stage(k)
        if k == 5:
            pl.semaphore_wait(level.at[0], 4)
            pass_on(1)
        send(k)

    for i in range(8):
        load_probes(i).start()
    prints[...] = jnp.zeros_like(prints)

    held_block = jnp.broadcast_to(block_row[...].astype(F32), (128, 128)).T
    shard = lax.broadcasted_iota(jnp.int32, (128, 128), 0)
    rep, tp = lax.div(shard, 32), lax.rem(shard, 32)
    src_x = lax.div(rep, 2) * 2 + lax.rem(lax.div(tp, 4), 2)
    where = slot(lax.div(tp, 8) * 4 + lax.rem(tp, 4), lax.rem(rep, 2), src_x)
    hit = held_block == lax.broadcasted_iota(jnp.int32, (128, 128), 1).astype(F32)
    slot_row[...] = jnp.sum(
        jnp.where(hit, where.astype(F32), 0.0), axis=0, keepdims=True
    ).astype(jnp.int32)
    to_scalar = pltpu.make_async_copy(slot_row, slot_of, map_sem.at[0])
    to_scalar.start()

    half = lax.div(lax.broadcasted_iota(jnp.int32, (128, 256), 0), 64)

    lane_half = lax.div(lax.broadcasted_iota(jnp.int32, (768, 128), 1), 64)

    def arrange(k, src_core, at_half):
        plane = plane_of(k)
        src_z, src_y = lax.div(plane, 4), lax.rem(plane, 4)
        for pair in range(2):
            ats, qs, os = [], [], []
            for src_x in (2 * pair, 2 * pair + 1):
                shard = ((src_x // 2) * 2 + src_core) * 32 + src_z * 8 + (src_x % 2) * 4 + src_y
                at_slot = slot(plane, src_core, src_x)
                q, o = recv[at_slot, 0:64, :], recv[at_slot, 64:128, :]
                q, o = (jnp.concatenate([part, part], axis=0) for part in (q, o))
                turned[at_slot] = o.T
                ats.append(block[0, shard])
                qs.append(q)
                os.append(o)
            side = lax.rem(ats[0], 2)
            one, two = (probes_v[:, lax.div(at, 2)].reshape(768, 128) for at in ats)
            swapped = pltpu.roll(two, 64, axis=1)
            two = jnp.where(lane_half * 0 + side == lax.rem(ats[1], 2), swapped, two)
            rows = slice(at_half * 256 + pair * 128, at_half * 256 + (pair + 1) * 128)
            lhs[:, rows] = jnp.where(lane_half == side, one, two)
            rhs[rows, 0:256] = jnp.where(half == side, *qs)
            rhs[rows, 256:512] = jnp.where(half == side, *os)

    def accumulate():
        @pl.loop(0, 2)
        def _(m):
            rows = pl.ds(pl.multiple_of(m * 384, 384), 384)
            prints[rows, :] += jnp.dot(lhs[rows, :], rhs[...], preferred_element_type=F32)

    def turn(t):
        y_swap, z_swap = ((at == 0).astype(jnp.int32) * 2 for at in (y, z))
        first, second, third, fourth = ((t == n).astype(jnp.int32) for n in (1, 2, 3, 4))
        return t + y_swap * (first - third) + z_swap * (second - fourth)

    @pl.loop(0, ROUNDS + LAG_D)
    def _(t):
        @pl.when((t >= 1) & (t + AHEAD < ROUNDS))
        def _():
            stage(t + AHEAD)

            if AHEAD < 5:
                @pl.when(t + AHEAD == 5)
                def _():
                    pl.semaphore_wait(level.at[0], 4)
                    pass_on(1)

            @pl.when(t + AHEAD == 11)
            def _():
                pl.semaphore_wait(level.at[1], 4)
                pass_on(2)

            @pl.when(t + AHEAD == 15)
            def _():
                pl.semaphore_wait(level.at[2], 4)

            send(t + AHEAD)

        @pl.when((t >= 1) & (t < ROUNDS))
        def _():
            k = turn(t)
            far(k).wait_recv()
            first, second, third = along(k)
            first.start()
            second.start()
            near(k).wait_recv()
            third.start()

        @pl.when((t >= LAG_X) & (t < ROUNDS + LAG_X))
        def _():
            for copy in along(turn(t - LAG_X)):
                copy.wait_recv()
            across(turn(t - LAG_X)).start()

            @pl.when(t == LAG_X)
            def _():
                for i in range(8):
                    load_probes(i).wait()

        @pl.when(t >= LAG_D)
        def _():
            across(turn(t - LAG_D)).wait_recv()
            arrange(turn(t - LAG_D), 1 - core, 1)
            accumulate()

        @pl.when((t >= LAG_X) & (t < ROUNDS + LAG_X))
        def _():
            arrange(turn(t - LAG_X), core, 0)

    to_scalar.wait()

    @pl.loop(0, ROUNDS)
    def _(k):
        @pl.when(k >= 1)
        def _():
            near(k).wait_send()
            far(k).wait_send()

        for copy in along(k):
            copy.wait_send()
        across(k).wait_send()


def place_kernel(slot_of, recv, turned, prints, q_out, o_out, qp_out, op_out,
                 o_all, op_all, sems):
    qp = pltpu.make_async_copy(prints.at[:, 0:256], qp_out, sems.at[1])
    qp.start()
    left = lax.broadcasted_iota(jnp.int32, (256, 128), 1) < 64
    outs = []
    for part in range(4):
        @pl.loop(part * 16, (part + 1) * 16)
        def _(p):
            slots = slot_of[0, 2 * p], slot_of[0, 2 * p + 1]
            for i in (0, 1):
                rows = pl.ds(pl.multiple_of(p * 128 + i * 64, 64), 64)
                pltpu.make_async_copy(
                    recv.at[slots[i], 0:64, :], q_out.at[rows, :], sems.at[0]
                ).start()
            cols = pl.ds(pl.multiple_of(p * 128, 128), 128)
            o_all[:, cols] = jnp.where(left, turned[slots[0]], turned[slots[1]])

        cols = slice(part * 2048, (part + 1) * 2048)
        copy = pltpu.make_async_copy(o_all.at[:, cols], o_out.at[:, cols], sems.at[3 + part])
        copy.start()
        outs.append(copy)
    op_all[...] = prints[:, 256:512].T
    op = pltpu.make_async_copy(op_all, op_out, sems.at[2])
    op.start()
    for copy in [qp, op] + outs:
        copy.wait()
    pltpu.make_async_copy(q_out, q_out, sems.at[0]).wait()


def tiles(shard):
    return shard.reshape(8, 8, 32, 2, 128).transpose(0, 2, 3, 1, 4)


def per_device(trainer_query, trainer_output, probes, shard_block, slice_owner):
    smem = pl.BlockSpec(memory_space=pltpu.SMEM)
    hbm = pl.BlockSpec(memory_space=pltpu.HBM)
    vmem = pl.BlockSpec(memory_space=pltpu.VMEM)
    dma = pltpu.SemaphoreType.DMA

    def in_hbm(array):
        return pltpu.with_memory_space_constraint(array, pltpu.HBM)

    recv, turned, prints, slot_of = pl.pallas_call(
        move_kernel,
        out_shape=(
            pltpu.VMEM((128, 128, 256), BF16),
            pltpu.VMEM((128, 256, 128), BF16),
            pltpu.VMEM((768, 512), F32),
            pltpu.SMEM((1, 128), jnp.int32),
        ),
        in_specs=[hbm, hbm, hbm, hbm, hbm],
        out_specs=(vmem, vmem, vmem, smem),
        scratch_shapes=[
            pltpu.SMEM((32,), jnp.int32),
            pltpu.SMEM((1, 128), jnp.int32),
            pltpu.VMEM((1, 128), jnp.int32),
            pltpu.VMEM((1, 128), jnp.int32),
            pltpu.VMEM((8, 32, 2, 8, 128), F32),
            pltpu.VMEM((8, 32, 2, 8, 128), F32),
            pltpu.VMEM((96, 64, 8, 128), BF16),
            pltpu.VMEM((ROUNDS, 2, 128, 256), BF16),
            pltpu.VMEM((ROUNDS, 128, 256), BF16),
            pltpu.VMEM((768, 512), BF16),
            pltpu.VMEM((512, 512), BF16),
            pltpu.SemaphoreType.REGULAR((3,)), dma((3,)), dma((2, 8)), dma((8,)), dma((ROUNDS,)), dma((ROUNDS,)), dma((ROUNDS,)), dma((ROUNDS,)),
            dma((ROUNDS, 3)), dma((ROUNDS, 3)), dma((ROUNDS,)), dma((ROUNDS,)),
        ],
        compiler_params=pltpu.CompilerParams(
            collective_id=0, has_side_effects=True, vmem_limit_bytes=30 << 20
        ),
        name="move",
    )(
        in_hbm(slice_owner),
        in_hbm(shard_block.reshape(1, 128)),
        in_hbm(tiles(trainer_query[0])),
        in_hbm(tiles(jnp.swapaxes(trainer_output, 1, 2)[0])),
        in_hbm(probes.reshape(96, 8, 64, 128).transpose(0, 2, 1, 3)),
    )
    outs = pl.pallas_call(
        place_kernel,
        out_shape=(
            jax.ShapeDtypeStruct((8192, 256), BF16),
            jax.ShapeDtypeStruct((256, 8192), BF16),
            jax.ShapeDtypeStruct((768, 256), F32),
            jax.ShapeDtypeStruct((256, 768), F32),
        ),
        in_specs=[smem, vmem, vmem, vmem],
        out_specs=(hbm, hbm, hbm, hbm),
        scratch_shapes=[
            pltpu.VMEM((256, 8192), BF16),
            pltpu.VMEM((256, 768), F32),
            dma((8,)),
        ],
        compiler_params=pltpu.CompilerParams(vmem_limit_bytes=10 << 20),
        name="place",
    )(slot_of, recv, turned, prints)
    return tuple(out[None] for out in outs)


def solution(mesh):
    placed = (P(("rep", "tp"), None, None), P(("rep", "tp"), None, None), P(), P(), P())
    return jax.shard_map(
        per_device,
        mesh=mesh,
        in_specs=placed,
        out_specs=(
            P("tp", None, None),
            P("tp", None, None),
            P("tp", None, None),
            P("tp", None, None),
        ),
        check_vma=False,
    )
```

```python
import jax
import jax.numpy as jnp
from jax import lax
from jax.experimental import pallas as pl
from jax.experimental.pallas import tpu as pltpu
from jax.sharding import PartitionSpec as P

MESH = pl.DeviceIdType.MESH
BF16 = jnp.bfloat16
F32 = jnp.float32

ROUNDS = 16
LAG_X = 3
LAG_D = 4
AHEAD = 6


STEPS = (
    (0, 0), (1, 0), (0, 1), (3, 0), (0, 3), (1, 1), (3, 3), (2, 0),
    (1, 3), (3, 1), (0, 2), (2, 1), (1, 2), (2, 3), (3, 2), (2, 2),
)


def offset_of(k):
    k = jnp.int32(k)
    return tuple(
        sum(steps[i] * (k == n).astype(jnp.int32) for n, steps in enumerate(STEPS) if steps[i])
        for i in (0, 1)
    )


def place():
    rep, tp = lax.axis_index("rep"), lax.axis_index("tp")
    x = lax.div(rep, 2) * 2 + lax.rem(lax.div(tp, 4), 2)
    return x, lax.rem(tp, 4), lax.div(tp, 8), lax.rem(rep, 2)


def device(x, y, z, core):
    x, y, z = lax.rem(x, 4), lax.rem(y, 4), lax.rem(z, 4)
    return {"rep": lax.div(x, 2) * 2 + core, "tp": z * 8 + lax.rem(x, 2) * 4 + y}


def move_kernel(
    owner_hbm, block_hbm, query, output, probes,
    recv, turned, prints, slot_of,
    owner, block, block_row, slot_row, query_f, output_f, probes_v, staged, relay, lhs, rhs,
    level, map_sem, load_sem, probe_sem, near_s, near_r, far_s, far_r, x_s, x_r, d_s, d_r,
):
    x, y, z, core = place()
    mine = z * 4 + y
    barrier = pltpu.get_barrier_semaphore()
    beside = [device(x, y + dy, z + dz, core) for dy, dz in ((1, 0), (3, 0), (0, 1), (0, 3))]
    peers = [device(x + d, y, z, core) for d in (1, 2, 3)] + [device(x, y, z, 1 - core)] + beside

    for peer in peers:
        pl.semaphore_signal(barrier, 1, device_id=peer, device_id_type=MESH)

    def load(kind, i):
        src, dst = ((query, query_f), (output, output_f))[kind]
        return pltpu.make_async_copy(src.at[i], dst.at[i], load_sem.at[kind, i])

    def load_probes(i):
        rows = pl.ds(i * 12, 12)
        return pltpu.make_async_copy(probes.at[rows], probes_v.at[rows], probe_sem.at[i])

    maps = [
        pltpu.make_async_copy(owner_hbm, owner, map_sem.at[0]),
        pltpu.make_async_copy(block_hbm, block, map_sem.at[1]),
        pltpu.make_async_copy(block_hbm, block_row, map_sem.at[2]),
    ]
    for copy in maps:
        copy.start()
    for i in range(8):
        load(0, i).start()
        load(1, i).start()
    def remote(src, dst, send, receive, target):
        return pltpu.make_async_remote_copy(
            src_ref=src, dst_ref=dst, send_sem=send, recv_sem=receive,
            device_id=target, device_id_type=MESH,
        )

    def plane_of(k):
        dy, dz = offset_of(k)
        return lax.rem(z - dz + 4, 4) * 4 + lax.rem(y - dy + 4, 4)

    def slot(plane, src_core, src_x):
        return plane * 8 + src_core * 4 + src_x

    def near(k):
        dy, dz = offset_of(k)
        return remote(staged.at[k, 0], recv.at[slot(mine, core, x)], near_s.at[k], near_r.at[k],
                      device(x, y + dy, z + dz, core))

    def far(k):
        dy, dz = offset_of(k)
        return remote(staged.at[k, 1], relay.at[k], far_s.at[k], far_r.at[k],
                      device(x, y + dy, z + dz, core))

    def along(k):
        own = recv.at[slot(plane_of(k), core, x)]
        return (
            remote(relay.at[k], own, x_s.at[k, 0], x_r.at[k, 0], device(x + 1, y, z, core)),
            remote(relay.at[k], own, x_s.at[k, 1], x_r.at[k, 1], device(x + 3, y, z, core)),
            remote(own, own, x_s.at[k, 2], x_r.at[k, 2], device(x + 2, y, z, core)),
        )

    def across(k):
        half = recv.at[pl.ds(slot(plane_of(k), core, 0), 4)]
        return remote(half, half, d_s.at[k], d_r.at[k], device(x, y, z, 1 - core))

    def piece(source, k, other, part):
        dy, dz = offset_of(k)
        low = lax.rem(x + other, 2)
        j = lax.rem(z + dz, 4) * 8 + low * 4 + lax.rem(y + dy, 4)
        return source[:, owner[j], part].reshape(64, 128).astype(BF16)

    def cut(dst, k, other):
        for row, source in ((0, query_f), (64, output_f)):
            for part in (0, 1):
                dst[row : row + 64, part * 128 : (part + 1) * 128] = piece(source, k, other, part)

    def stage(k):
        for other in (0, 1):
            cut(staged.at[k, other], k, other)

    def send(k):
        far(k).start()
        near(k).start()

    def pass_on(i):
        for peer in beside:
            pl.semaphore_signal(level.at[i], 1, device_id=peer, device_id_type=MESH)

    for copy in maps:
        copy.wait()
    for i in range(8):
        load(0, i).wait()
        load(1, i).wait()
    cut(recv.at[slot(mine, core, x)], 0, 0)
    cut(relay.at[0], 0, 1)
    stage(1)
    pl.semaphore_wait(barrier, len(peers))
    for copy in along(0):
        copy.start()
    send(1)
    pass_on(0)
    for k in range(2, AHEAD + 1):
        stage(k)
        if k == 5:
            pl.semaphore_wait(level.at[0], 4)
            pass_on(1)
        send(k)

    for i in range(8):
        load_probes(i).start()
    prints[...] = jnp.zeros_like(prints)

    held_block = jnp.broadcast_to(block_row[...].astype(F32), (128, 128)).T
    shard = lax.broadcasted_iota(jnp.int32, (128, 128), 0)
    rep, tp = lax.div(shard, 32), lax.rem(shard, 32)
    src_x = lax.div(rep, 2) * 2 + lax.rem(lax.div(tp, 4), 2)
    where = slot(lax.div(tp, 8) * 4 + lax.rem(tp, 4), lax.rem(rep, 2), src_x)
    hit = held_block == lax.broadcasted_iota(jnp.int32, (128, 128), 1).astype(F32)
    slot_row[...] = jnp.sum(
        jnp.where(hit, where.astype(F32), 0.0), axis=0, keepdims=True
    ).astype(jnp.int32)
    to_scalar = pltpu.make_async_copy(slot_row, slot_of, map_sem.at[0])
    to_scalar.start()

    half = lax.div(lax.broadcasted_iota(jnp.int32, (128, 256), 0), 64)

    lane_half = lax.div(lax.broadcasted_iota(jnp.int32, (768, 128), 1), 64)

    def arrange(k, src_core, at_half):
        plane = plane_of(k)
        src_z, src_y = lax.div(plane, 4), lax.rem(plane, 4)
        for pair in range(2):
            ats, qs, os = [], [], []
            for src_x in (2 * pair, 2 * pair + 1):
                shard = ((src_x // 2) * 2 + src_core) * 32 + src_z * 8 + (src_x % 2) * 4 + src_y
                at_slot = slot(plane, src_core, src_x)
                q, o = recv[at_slot, 0:64, :], recv[at_slot, 64:128, :]
                q, o = (jnp.concatenate([part, part], axis=0) for part in (q, o))
                turned[at_slot] = o.T
                ats.append(block[0, shard])
                qs.append(q)
                os.append(o)
            side = lax.rem(ats[0], 2)
            one, two = (probes_v[:, lax.div(at, 2)].reshape(768, 128) for at in ats)
            swapped = pltpu.roll(two, 64, axis=1)
            two = jnp.where(lane_half * 0 + side == lax.rem(ats[1], 2), swapped, two)
            rows = slice(at_half * 256 + pair * 128, at_half * 256 + (pair + 1) * 128)
            lhs[:, rows] = jnp.where(lane_half == side, one, two)
            rhs[rows, 0:256] = jnp.where(half == side, *qs)
            rhs[rows, 256:512] = jnp.where(half == side, *os)

    def accumulate():
        prints[...] += jnp.dot(lhs[...], rhs[...], preferred_element_type=F32)

    def turn(t):
        y_swap, z_swap = ((at == 0).astype(jnp.int32) * 2 for at in (y, z))
        first, second, third, fourth = ((t == n).astype(jnp.int32) for n in (1, 2, 3, 4))
        return t + y_swap * (first - third) + z_swap * (second - fourth)

    @pl.loop(0, ROUNDS + LAG_D)
    def _(t):
        @pl.when((t >= 1) & (t + AHEAD < ROUNDS))
        def _():
            stage(t + AHEAD)

            if AHEAD < 5:
                @pl.when(t + AHEAD == 5)
                def _():
                    pl.semaphore_wait(level.at[0], 4)
                    pass_on(1)

            @pl.when(t + AHEAD == 11)
            def _():
                pl.semaphore_wait(level.at[1], 4)
                pass_on(2)

            @pl.when(t + AHEAD == 15)
            def _():
                pl.semaphore_wait(level.at[2], 4)

            send(t + AHEAD)

        @pl.when((t >= 1) & (t < ROUNDS))
        def _():
            k = turn(t)
            far(k).wait_recv()
            first, second, third = along(k)
            first.start()
            second.start()
            near(k).wait_recv()
            third.start()

        @pl.when((t >= LAG_X) & (t < ROUNDS + LAG_X))
        def _():
            for copy in along(turn(t - LAG_X)):
                copy.wait_recv()
            across(turn(t - LAG_X)).start()

            @pl.when(t == LAG_X)
            def _():
                for i in range(8):
                    load_probes(i).wait()

        @pl.when(t >= LAG_D)
        def _():
            across(turn(t - LAG_D)).wait_recv()
            arrange(turn(t - LAG_D), 1 - core, 1)
            accumulate()

        @pl.when((t >= LAG_X) & (t < ROUNDS + LAG_X))
        def _():
            arrange(turn(t - LAG_X), core, 0)

    to_scalar.wait()

    @pl.loop(0, ROUNDS)
    def _(k):
        @pl.when(k >= 1)
        def _():
            near(k).wait_send()
            far(k).wait_send()

        for copy in along(k):
            copy.wait_send()
        across(k).wait_send()


def place_kernel(slot_of, recv, turned, prints, q_out, o_out, qp_out, op_out,
                 o_all, op_all, sems):
    qp = pltpu.make_async_copy(prints.at[:, 0:256], qp_out, sems.at[1])
    qp.start()
    left = lax.broadcasted_iota(jnp.int32, (256, 128), 1) < 64
    outs = []
    for part in range(4):
        @pl.loop(part * 16, (part + 1) * 16)
        def _(p):
            slots = slot_of[0, 2 * p], slot_of[0, 2 * p + 1]
            for i in (0, 1):
                rows = pl.ds(pl.multiple_of(p * 128 + i * 64, 64), 64)
                pltpu.make_async_copy(
                    recv.at[slots[i], 0:64, :], q_out.at[rows, :], sems.at[0]
                ).start()
            cols = pl.ds(pl.multiple_of(p * 128, 128), 128)
            o_all[:, cols] = jnp.where(left, turned[slots[0]], turned[slots[1]])

        cols = slice(part * 2048, (part + 1) * 2048)
        copy = pltpu.make_async_copy(o_all.at[:, cols], o_out.at[:, cols], sems.at[3 + part])
        copy.start()
        outs.append(copy)
    op_all[...] = prints[:, 256:512].T
    op = pltpu.make_async_copy(op_all, op_out, sems.at[2])
    op.start()
    for copy in [qp, op] + outs:
        copy.wait()
    pltpu.make_async_copy(q_out, q_out, sems.at[0]).wait()


def tiles(shard):
    return shard.reshape(8, 8, 32, 2, 128).transpose(0, 2, 3, 1, 4)


def per_device(trainer_query, trainer_output, probes, shard_block, slice_owner):
    smem = pl.BlockSpec(memory_space=pltpu.SMEM)
    hbm = pl.BlockSpec(memory_space=pltpu.HBM)
    vmem = pl.BlockSpec(memory_space=pltpu.VMEM)
    dma = pltpu.SemaphoreType.DMA

    def in_hbm(array):
        return pltpu.with_memory_space_constraint(array, pltpu.HBM)

    recv, turned, prints, slot_of = pl.pallas_call(
        move_kernel,
        out_shape=(
            pltpu.VMEM((128, 128, 256), BF16),
            pltpu.VMEM((128, 256, 128), BF16),
            pltpu.VMEM((768, 512), F32),
            pltpu.SMEM((1, 128), jnp.int32),
        ),
        in_specs=[hbm, hbm, hbm, hbm, hbm],
        out_specs=(vmem, vmem, vmem, smem),
        scratch_shapes=[
            pltpu.SMEM((32,), jnp.int32),
            pltpu.SMEM((1, 128), jnp.int32),
            pltpu.VMEM((1, 128), jnp.int32),
            pltpu.VMEM((1, 128), jnp.int32),
            pltpu.VMEM((8, 32, 2, 8, 128), F32),
            pltpu.VMEM((8, 32, 2, 8, 128), F32),
            pltpu.VMEM((96, 64, 8, 128), BF16),
            pltpu.VMEM((ROUNDS, 2, 128, 256), BF16),
            pltpu.VMEM((ROUNDS, 128, 256), BF16),
            pltpu.VMEM((768, 512), BF16),
            pltpu.VMEM((512, 512), BF16),
            pltpu.SemaphoreType.REGULAR((3,)), dma((3,)), dma((2, 8)), dma((8,)), dma((ROUNDS,)), dma((ROUNDS,)), dma((ROUNDS,)), dma((ROUNDS,)),
            dma((ROUNDS, 3)), dma((ROUNDS, 3)), dma((ROUNDS,)), dma((ROUNDS,)),
        ],
        compiler_params=pltpu.CompilerParams(
            collective_id=0, has_side_effects=True, vmem_limit_bytes=30 << 20
        ),
        name="move",
    )(
        in_hbm(slice_owner),
        in_hbm(shard_block.reshape(1, 128)),
        in_hbm(tiles(trainer_query[0])),
        in_hbm(tiles(jnp.swapaxes(trainer_output, 1, 2)[0])),
        in_hbm(probes.reshape(96, 8, 64, 128).transpose(0, 2, 1, 3)),
    )
    outs = pl.pallas_call(
        place_kernel,
        out_shape=(
            jax.ShapeDtypeStruct((8192, 256), BF16),
            jax.ShapeDtypeStruct((256, 8192), BF16),
            jax.ShapeDtypeStruct((768, 256), F32),
            jax.ShapeDtypeStruct((256, 768), F32),
        ),
        in_specs=[smem, vmem, vmem, vmem],
        out_specs=(hbm, hbm, hbm, hbm),
        scratch_shapes=[
            pltpu.VMEM((256, 8192), BF16),
            pltpu.VMEM((256, 768), F32),
            dma((8,)),
        ],
        compiler_params=pltpu.CompilerParams(vmem_limit_bytes=10 << 20),
        name="place",
    )(slot_of, recv, turned, prints)
    return tuple(out[None] for out in outs)


def solution(mesh):
    placed = (P(("rep", "tp"), None, None), P(("rep", "tp"), None, None), P(), P(), P())
    return jax.shard_map(
        per_device,
        mesh=mesh,
        in_specs=placed,
        out_specs=(
            P("tp", None, None),
            P("tp", None, None),
            P("tp", None, None),
            P("tp", None, None),
        ),
        check_vma=False,
    )
```
